32 devices in a mesh: vocab: 8 (over z, x), seq: 4 (over y, core).
Axes of the slice: x: 2, y: 2, z: 4, core: 2. Of those that a mesh axis runs over, the one named last changes fastest.
Arguments:
- hidden: bfloat16 [1536, 7168], P(('vocab', 'seq')), may hold values from -64 to 64
- head_matrix: bfloat16 [7168, 8192], P('seq', 'vocab'), may hold values from -4 to 4
- targets: int32 [1536], P(('vocab', 'seq')), may hold values from 0 to 8191
Outputs:
- logprob: float32 [1536], P(('vocab', 'seq'))
The draws below stay inside these ranges and needn't reach their ends.
All inputs are finite; a program needn't handle non-finite values.
Results may differ from the reference program's by a relative error of at most 0.0003.
Values may be sent and summed in bfloat16 or wider, within the bound.
A program may use at most 128 MiB of HBM per device.

```python
import math
import jax
import jax.numpy as jnp
from jax import lax

D = 7168
TOK_DEV = 48
VOCAB = 8192
TOKENS = 1536
N_SEQ = 4


def head_column(key, column):
    values = jax.random.normal(jax.random.fold_in(jax.random.fold_in(key, 11), column), (D,), jnp.float32)
    values = jnp.clip(values, -4.0, 4.0)
    spread = jax.random.uniform(jax.random.fold_in(jax.random.fold_in(key, 12), column), (), jnp.float32, -0.7, 0.7)
    return values * jnp.exp(spread) * 3.0 / math.sqrt(D)


def head_columns(key, columns):

    def single(column):
        return head_column(key, column)
    return jax.vmap(single)(columns)


def draw_head_matrix(key, part):
    return head_columns(key, jnp.arange(VOCAB)).T.astype(jnp.bfloat16)


def draw_hidden(key, part):
    base_key = jax.random.fold_in(key, 21)
    return jax.random.normal(base_key, (TOKENS, D), jnp.float32).astype(jnp.bfloat16)


def with_ends(drawn, stream_key, least, high):
    spot = [jax.random.randint(jax.random.fold_in(stream_key, axis), (), 0, length) for axis, length in enumerate(drawn.shape)]
    widest = drawn.shape.index(max(drawn.shape))
    neighbour = spot[:widest] + [(spot[widest] + 1) % drawn.shape[widest]] + spot[widest + 1:]
    return drawn.at[tuple(spot)].set(least).at[tuple(neighbour)].set(high)


def setup_inputs(seed: int = 0) -> dict:
    splits = jax.random.split(jax.random.key(seed), 4)
    return {
        "hidden": draw_hidden(jax.random.fold_in(splits[3], 71), 0),
        "head_matrix": draw_head_matrix(jax.random.fold_in(splits[3], 71), 0),
        "targets": with_ends(jax.random.randint(splits[2], (TOKENS,), 0, VOCAB), jax.random.fold_in(splits[2], 1), 0, VOCAB - 1).astype(jnp.int32),
    }


def block_logprob(rows, wanted, head_matrix):
    logits = jnp.dot(rows, head_matrix, preferred_element_type=jnp.float32)
    maximum = jnp.max(logits, axis=1)
    log_total = maximum + jnp.log(jnp.sum(jnp.exp(logits - maximum[:, None]), axis=1))
    picked = jnp.take_along_axis(logits, wanted[:, None].astype(jnp.int32), axis=1)[:, 0]
    return picked - log_total


def reference(hidden, head_matrix, targets):
    block_rows = TOK_DEV * N_SEQ
    block_count = hidden.shape[0] // block_rows
    rows = hidden.reshape(block_count, block_rows, hidden.shape[1])
    wanted = targets.reshape(block_count, block_rows)

    def one_block(pieces):
        return block_logprob(pieces[0], pieces[1], head_matrix)

    results = lax.map(one_block, (rows, wanted))
    return results.reshape(-1)
```

```python
import functools

import jax
import jax.numpy as jnp
from jax import lax
from jax.experimental import pallas as pl
from jax.experimental.pallas import tpu as pltpu
from jax.sharding import PartitionSpec as P

MESH = pl.DeviceIdType.MESH
TILE = 256


def ring_index(position, n):
    half = n // 2
    p = lax.rem(position + 2 * n, n)
    low = p // half
    high = jnp.where(low == 0, p, n - 1 - p)
    return high * 2 + low


def kernel(
    n, hidden, head, targets, out,
    x, w, wanted, part, other, stats, gathered,
    local_sem, swap_tx, swap_rx, ring_tx, ring_rx, part_tx, part_rx, stat_tx, stat_rx,
):
    half = n // 2
    width = head.shape[0]
    columns = head.shape[1]
    rows = hidden.shape[0]
    tile = min(TILE, columns)
    v = lax.axis_index("vocab")
    s = lax.axis_index("seq")
    y, c = s // 2, lax.rem(s, 2)
    low, high = lax.rem(v, 2), v // 2
    position = jnp.where(low == 0, high, n - 1 - high)
    ring = ((ring_index(position + 1, n), s), (ring_index(position - 1, n), s))
    y_mate = (v, (1 - y) * 2 + c)
    c_mate = (v, y * 2 + 1 - c)

    barrier = pltpu.get_barrier_semaphore()
    for device in (*ring, y_mate, c_mate):
        pl.semaphore_signal(barrier, inc=1, device_id=device, device_id_type=MESH)
    pl.semaphore_wait(barrier, 4)

    def remote(src, dst, tx, rx, device):
        return pltpu.make_async_remote_copy(
            src_ref=src, dst_ref=dst, send_sem=tx, recv_sem=rx, device_id=device, device_id_type=MESH
        )

    def block_at(direction, d):
        return ring_index(position - d if direction == 0 else position + d, n)

    def chunk_ref(block, ch):
        if ch == 4:
            return wanted.at[block]
        unit = y if ch < 2 else 1 - y
        return x.at[block, ch % 2, unit]

    def hop(direction, d, ch, src=None):
        dst = chunk_ref(block_at(direction, d), ch)
        return remote(
            dst if src is None else src, dst,
            ring_tx.at[direction, d, ch], ring_rx.at[direction, d + 1, ch], ring[direction],
        )

    def arrived(direction, d, ch):
        dst = chunk_ref(block_at(direction, d), ch)
        remote(dst, dst, ring_tx.at[direction, d - 1, ch], ring_rx.at[direction, d, ch], ring[direction]).wait_recv()

    def hidden_piece(half_y, h):
        start = pl.multiple_of((half_y * 2 + h) * width, width)
        return hidden.at[:, pl.ds(start, width)]

    own = []
    for h in range(2):
        for direction in range(2):
            hop(direction, 0, h, hidden_piece(y, h)).start()
    swaps = [
        remote(hidden_piece(1 - y, h), x.at[v, h, y], swap_tx.at[h], swap_rx.at[h], y_mate) for h in range(2)
    ]
    for swap in swaps:
        swap.start()
    for direction in range(2):
        hop(direction, 0, 4, targets).start()
    head_swap = remote(head, w.at[c], swap_tx.at[2], swap_rx.at[2], c_mate)
    head_swap.start()
    own.append(pltpu.make_async_copy(head, w.at[c], local_sem.at[0]))
    own.append(pltpu.make_async_copy(targets, wanted.at[v], local_sem.at[1]))
    for h in range(2):
        own.append(pltpu.make_async_copy(hidden_piece(y, h), x.at[v, h, y], local_sem.at[2 + h]))
    for copy in own:
        copy.start()

    def multiply(block):
        @pl.loop(0, columns // tile)
        def _(j):
            at = pl.ds(pl.multiple_of(j * tile, tile), tile)
            total = None
            for h in range(2):
                term = jnp.dot(
                    x[block, h].reshape(2 * rows, width), w[h, :, at], preferred_element_type=jnp.float32
                )
                total = term if total is None else total + term
            part[block, :, :, at] = total.reshape(2, rows, tile)

    def multiply_unit(block, unit):
        @pl.loop(0, columns // tile)
        def _(j):
            at = pl.ds(pl.multiple_of(j * tile, tile), tile)
            total = None
            for h in range(2):
                term = jnp.dot(x[block, h, unit], w[h, :, at], preferred_element_type=jnp.float32)
                total = term if total is None else total + term
            part[block, unit, :, at] = total

    def part_copy(block):
        return remote(part.at[block, 1 - y], other.at[block], part_tx.at[block], part_rx.at[block], y_mate)

    def stat_copy(block):
        return remote(stats.at[block], gathered.at[v], stat_tx.at[block], stat_rx.at[v], (block, s))

    def row_stats(block):
        part_copy(block).wait_recv()
        logits = part[block, y] + other[block]
        maximum = jnp.max(logits, axis=1, keepdims=True)
        expsum = jnp.sum(jnp.exp(logits - maximum), axis=1, keepdims=True)
        diagonal = lax.broadcasted_iota(jnp.int32, (rows, rows), 0) == lax.broadcasted_iota(
            jnp.int32, (rows, rows), 1
        )
        target = jnp.sum(jnp.where(diagonal, wanted[block], 0), axis=1, keepdims=True)
        column = lax.broadcasted_iota(jnp.int32, logits.shape, 1) + v * columns
        picked = jnp.sum(jnp.where(column == target, logits, 0.0), axis=1, keepdims=True)
        maximum, expsum, picked = (
            jnp.sum(jnp.where(diagonal, values, 0.0), axis=0, keepdims=True)
            for values in (maximum, expsum, picked)
        )
        line = lax.broadcasted_iota(jnp.int32, (8, rows), 0)
        return jnp.where(line == 0, maximum, jnp.where(line == 1, expsum, picked))

    def give_stats(block):
        stats[block] = row_stats(block)
        stat_copy(block).start()

    for h in range(2):
        swaps[h].wait_recv()
        for direction in range(2):
            hop(direction, 0, 2 + h).start()
    for copy in own:
        copy.wait()
    head_swap.wait_recv()
    multiply(v)
    part_copy(v).start()

    def step(d):
        for ch in (4, 0, 1, 2, 3):
            for direction in range(2):
                arrived(direction, d, ch)
                hop(direction, d, ch).start()

    def compute(d):
        for direction in range(2):
            block = block_at(direction, d)
            multiply(block)
            part_copy(block).start()

    step(1)
    compute(1)
    gathered[v] = row_stats(v)

    @pl.loop(2, half - 1)
    def _(d):
        step(d)
        compute(d)
        for direction in range(2):
            give_stats(block_at(direction, d - 1))

    last = half - 1
    final = ((4, 2, 0), (3, 1))
    for direction in range(2):
        arrived(direction, last, 4)
    hop(0, last, 4).start()
    for ch in (0, 1):
        for direction in range(2):
            arrived(direction, last, ch)
    for ch in (2, 3):
        for direction in range(2):
            arrived(direction, last, ch)
            if ch in final[direction]:
                hop(direction, last, ch).start()
    hop(0, last, 0).start()
    hop(1, last, 1).start()
    compute(last)
    for direction in range(2):
        give_stats(block_at(direction, last - 1))

    far = block_at(0, half)
    arrived(0, half, 4)
    arrived(0, half, 2)
    arrived(1, half, 3)
    multiply_unit(far, 1 - y)
    part_copy(far).start()
    for direction in range(2):
        give_stats(block_at(direction, last))
    arrived(0, half, 0)
    arrived(1, half, 1)
    multiply_unit(far, y)
    give_stats(far)

    for swap in (*swaps, head_swap):
        swap.wait_send()

    @pl.loop(0, last)
    def _(d):
        for direction in range(2):
            for ch in range(5):
                hop(direction, d, ch).wait_send()

    for direction in range(2):
        for ch in final[direction]:
            hop(direction, last, ch).wait_send()

    @pl.loop(0, n)
    def _(block):
        part_copy(block).wait_send()

    @pl.loop(1, n)
    def _(d):
        stat_copy(block_at(0, d)).wait_send()
        peer = block_at(0, d)
        remote(
            stats.at[peer], gathered.at[peer], stat_tx.at[peer], stat_rx.at[peer], (peer, s)
        ).wait_recv()

    maxima, expsums, picked = (gathered[:, i, :] for i in range(3))
    maximum = jnp.max(maxima, axis=0, keepdims=True)
    expsum = jnp.sum(expsums * jnp.exp(maxima - maximum), axis=0, keepdims=True)
    out[...] = jnp.sum(picked, axis=0, keepdims=True) - (maximum + jnp.log(expsum))


def local(hidden, head_matrix, targets):
    n = lax.axis_size("vocab")
    half = n // 2
    rows = hidden.shape[0]
    width, columns = head_matrix.shape
    dma = pltpu.SemaphoreType.DMA
    result = pl.pallas_call(
        functools.partial(kernel, n),
        out_shape=jax.ShapeDtypeStruct((1, rows), jnp.float32),
        in_specs=[pl.BlockSpec(memory_space=pl.ANY)] * 3,
        out_specs=pl.BlockSpec(memory_space=pltpu.VMEM),
        scratch_shapes=[
            pltpu.VMEM((n, 2, 2, rows, width), jnp.bfloat16),
            pltpu.VMEM((2, width, columns), jnp.bfloat16),
            pltpu.VMEM((n, 1, rows), jnp.int32),
            pltpu.VMEM((n, 2, rows, columns), jnp.float32),
            pltpu.VMEM((n, rows, columns), jnp.float32),
            pltpu.VMEM((n, 8, rows), jnp.float32),
            pltpu.VMEM((n, 8, rows), jnp.float32),
            dma((4,)),
            dma((3,)),
            dma((3,)),
            dma((2, half, 5)),
            dma((2, half + 1, 5)),
            dma((n,)),
            dma((n,)),
            dma((n,)),
            dma((n,)),
        ],
        compiler_params=pltpu.CompilerParams(
            collective_id=0, has_side_effects=True, vmem_limit_bytes=62 * 1024 * 1024
        ),
    )(hidden, head_matrix, targets.reshape(1, rows))
    return result.reshape(rows)


def solution(mesh):
    return jax.shard_map(
        local,
        mesh=mesh,
        in_specs=(P(("vocab", "seq"), None), P("seq", "vocab"), P(("vocab", "seq"))),
        out_specs=P(("vocab", "seq")),
        check_vma=False,
    )
```

```python
import functools

import jax
import jax.numpy as jnp
from jax import lax
from jax.experimental import pallas as pl
from jax.experimental.pallas import tpu as pltpu
from jax.sharding import PartitionSpec as P

MESH = pl.DeviceIdType.MESH
TILE = 256


def ring_index(position, n):
    half = n // 2
    p = lax.rem(position + 2 * n, n)
    low = p // half
    high = jnp.where(low == 0, p, n - 1 - p)
    return high * 2 + low


def kernel(
    n, hidden, head, targets, out,
    x, w, wanted, part, other, stats, gathered,
    local_sem, swap_tx, swap_rx, ring_tx, ring_rx, part_tx, part_rx, far_tx, far_rx, stat_tx, stat_rx,
):
    half = n // 2
    width = head.shape[0]
    columns = head.shape[1]
    rows = hidden.shape[0]
    tile = min(TILE, columns)
    v = lax.axis_index("vocab")
    s = lax.axis_index("seq")
    y, c = s // 2, lax.rem(s, 2)
    low, high = lax.rem(v, 2), v // 2
    position = jnp.where(low == 0, high, n - 1 - high)
    ring = ((ring_index(position + 1, n), s), (ring_index(position - 1, n), s))
    y_mate = (v, (1 - y) * 2 + c)
    c_mate = (v, y * 2 + 1 - c)

    barrier = pltpu.get_barrier_semaphore()
    for device in (*ring, y_mate, c_mate):
        pl.semaphore_signal(barrier, inc=1, device_id=device, device_id_type=MESH)

    def remote(src, dst, tx, rx, device):
        return pltpu.make_async_remote_copy(
            src_ref=src, dst_ref=dst, send_sem=tx, recv_sem=rx, device_id=device, device_id_type=MESH
        )

    def block_at(direction, d):
        return ring_index(position - d if direction == 0 else position + d, n)

    def chunk_ref(block, ch):
        if ch == 4:
            return wanted.at[block]
        unit = y if ch < 2 else 1 - y
        return x.at[block, ch % 2, unit]

    def hop(direction, d, ch, src=None):
        dst = chunk_ref(block_at(direction, d), ch)
        return remote(
            dst if src is None else src, dst,
            ring_tx.at[direction, d, ch], ring_rx.at[direction, d + 1, ch], ring[direction],
        )

    def arrived(direction, d, ch):
        dst = chunk_ref(block_at(direction, d), ch)
        remote(dst, dst, ring_tx.at[direction, d - 1, ch], ring_rx.at[direction, d, ch], ring[direction]).wait_recv()

    def hidden_piece(half_y, h):
        start = pl.multiple_of((half_y * 2 + h) * width, width)
        return hidden.at[:, pl.ds(start, width)]

    own = [
        pltpu.make_async_copy(head, w.at[c], local_sem.at[0]),
        pltpu.make_async_copy(targets, wanted.at[v], local_sem.at[1]),
    ]
    for h in range(2):
        own.append(pltpu.make_async_copy(hidden_piece(y, h), x.at[v, h, y], local_sem.at[2 + h]))
    for copy in own:
        copy.start()
    pl.semaphore_wait(barrier, 4)
    for h in range(2):
        for direction in range(2):
            hop(direction, 0, h, hidden_piece(y, h)).start()
    swaps = [
        remote(hidden_piece(1 - y, h), x.at[v, h, y], swap_tx.at[h], swap_rx.at[h], y_mate) for h in range(2)
    ]
    for swap in swaps:
        swap.start()
    for direction in range(2):
        hop(direction, 0, 4, targets).start()
    head_swap = remote(head, w.at[c], swap_tx.at[2], swap_rx.at[2], c_mate)
    head_swap.start()

    def multiply(block):
        @pl.loop(0, columns // tile)
        def _(j):
            at = pl.ds(pl.multiple_of(j * tile, tile), tile)
            total = None
            for h in range(2):
                term = jnp.dot(
                    x[block, h].reshape(2 * rows, width), w[h, :, at], preferred_element_type=jnp.float32
                )
                total = term if total is None else total + term
            part[block, :, :, at] = total.reshape(2, rows, tile)

    def multiply_tile(blocks, unit, j):
        at = pl.ds(j * tile if isinstance(j, int) else pl.multiple_of(j * tile, tile), tile)
        total = None
        for h in range(2):
            lines = [x[block, h, unit] for block in blocks]
            term = jnp.dot(
                lines[0] if len(lines) == 1 else jnp.concatenate(lines, axis=0),
                w[h, :, at],
                preferred_element_type=jnp.float32,
            )
            total = term if total is None else total + term
        for i, block in enumerate(blocks):
            part[block, unit, :, at] = total[i * rows : (i + 1) * rows]

    def multiply_units(blocks, unit):
        @pl.loop(0, columns // tile)
        def _(j):
            multiply_tile(blocks, unit, j)

    def part_copy(block):
        return remote(part.at[block, 1 - y], other.at[block], part_tx.at[block], part_rx.at[block], y_mate)

    def far_copy(block, j):
        at = pl.ds(j * tile, tile)
        return remote(
            part.at[block, 1 - y, :, at], other.at[block, :, at], far_tx.at[j], far_rx.at[j], y_mate
        )

    def stat_copy(block):
        return remote(stats.at[block], gathered.at[v], stat_tx.at[block], stat_rx.at[v], (block, s))

    def row_stats(block):
        logits = part[block, y] + other[block]
        maximum = jnp.max(logits, axis=1, keepdims=True)
        expsum = jnp.sum(jnp.exp(logits - maximum), axis=1, keepdims=True)
        diagonal = lax.broadcasted_iota(jnp.int32, (rows, rows), 0) == lax.broadcasted_iota(
            jnp.int32, (rows, rows), 1
        )
        target = jnp.sum(jnp.where(diagonal, wanted[block], 0), axis=1, keepdims=True)
        column = lax.broadcasted_iota(jnp.int32, logits.shape, 1) + v * columns
        picked = jnp.sum(jnp.where(column == target, logits, 0.0), axis=1, keepdims=True)
        maximum, expsum, picked = (
            jnp.sum(jnp.where(diagonal, values, 0.0), axis=0, keepdims=True)
            for values in (maximum, expsum, picked)
        )
        line = lax.broadcasted_iota(jnp.int32, (8, rows), 0)
        return jnp.where(line == 0, maximum, jnp.where(line == 1, expsum, picked))

    def give_stats(block):
        part_copy(block).wait_recv()
        stats[block] = row_stats(block)
        stat_copy(block).start()

    for h in range(2):
        swaps[h].wait_recv()
        for direction in range(2):
            hop(direction, 0, 2 + h).start()
    for copy in own:
        copy.wait()
    head_swap.wait_recv()
    multiply(v)
    part_copy(v).start()

    def pass_on(d, chunks):
        for ch in chunks:
            for direction in range(2):
                arrived(direction, d, ch)
                hop(direction, d, ch).start()

    def pair(d):
        return [block_at(direction, d) for direction in range(2)]

    def compute_theirs(d):
        multiply_units(pair(d), 1 - y)
        for block in pair(d):
            part_copy(block).start()

    def compute_ours(d):
        multiply_units(pair(d), y)

    pass_on(1, (4, 0, 2, 1, 3))
    compute_theirs(1)
    compute_ours(1)
    part_copy(v).wait_recv()
    gathered[v] = row_stats(v)

    @pl.loop(2, half - 1)
    def _(d):
        pass_on(d, (4, 2, 3, 0, 1))
        compute_theirs(d)
        compute_ours(d)
        for block in pair(d - 1):
            give_stats(block)

    last = half - 1
    final = ((4, 2, 0), (3, 1))

    def pass_half(chunks):
        for ch in chunks:
            for direction in range(2):
                arrived(direction, last, ch)
                if ch in final[direction]:
                    hop(direction, last, ch).start()

    pass_half((4, 2, 3))
    compute_theirs(last)
    pass_half((0,))
    for block in pair(last - 1):
        give_stats(block)
    pass_half((1,))
    compute_ours(last)

    far = block_at(0, half)
    arrived(0, half, 4)
    arrived(0, half, 2)
    arrived(1, half, 3)
    for j in range(columns // tile):
        multiply_tile([far], 1 - y, j)
        if j > 0:
            far_copy(far, j - 1).start()
    far_copy(far, columns // tile - 1).start()
    for block in pair(last):
        give_stats(block)
    arrived(0, half, 0)
    arrived(1, half, 1)
    multiply_units([far], y)
    for j in range(columns // tile):
        far_copy(far, j).wait_recv()
    stats[far] = row_stats(far)
    stat_copy(far).start()

    for swap in (*swaps, head_swap):
        swap.wait_send()

    @pl.loop(0, last)
    def _(d):
        for direction in range(2):
            for ch in range(5):
                hop(direction, d, ch).wait_send()

    for direction in range(2):
        for ch in final[direction]:
            hop(direction, last, ch).wait_send()

    for j in range(columns // tile):
        far_copy(far, j).wait_send()
    part_copy(v).wait_send()

    @pl.loop(1, half)
    def _(d):
        for block in pair(d):
            part_copy(block).wait_send()

    @pl.loop(1, n)
    def _(d):
        stat_copy(block_at(0, d)).wait_send()
        peer = block_at(0, d)
        remote(
            stats.at[peer], gathered.at[peer], stat_tx.at[peer], stat_rx.at[peer], (peer, s)
        ).wait_recv()

    maxima, expsums, picked = (gathered[:, i, :] for i in range(3))
    maximum = jnp.max(maxima, axis=0, keepdims=True)
    expsum = jnp.sum(expsums * jnp.exp(maxima - maximum), axis=0, keepdims=True)
    out[...] = jnp.sum(picked, axis=0, keepdims=True) - (maximum + jnp.log(expsum))


def local(hidden, head_matrix, targets):
    n = lax.axis_size("vocab")
    half = n // 2
    rows = hidden.shape[0]
    width, columns = head_matrix.shape
    dma = pltpu.SemaphoreType.DMA
    result = pl.pallas_call(
        functools.partial(kernel, n),
        out_shape=jax.ShapeDtypeStruct((1, rows), jnp.float32),
        in_specs=[pl.BlockSpec(memory_space=pl.ANY)] * 3,
        out_specs=pl.BlockSpec(memory_space=pltpu.VMEM),
        scratch_shapes=[
            pltpu.VMEM((n, 2, 2, rows, width), jnp.bfloat16),
            pltpu.VMEM((2, width, columns), jnp.bfloat16),
            pltpu.VMEM((n, 1, rows), jnp.int32),
            pltpu.VMEM((n, 2, rows, columns), jnp.float32),
            pltpu.VMEM((n, rows, columns), jnp.float32),
            pltpu.VMEM((n, 8, rows), jnp.float32),
            pltpu.VMEM((n, 8, rows), jnp.float32),
            dma((4,)),
            dma((3,)),
            dma((3,)),
            dma((2, half, 5)),
            dma((2, half + 1, 5)),
            dma((n,)),
            dma((n,)),
            dma((columns // min(TILE, columns),)),
            dma((columns // min(TILE, columns),)),
            dma((n,)),
            dma((n,)),
        ],
        compiler_params=pltpu.CompilerParams(
            collective_id=0, has_side_effects=True, vmem_limit_bytes=62 * 1024 * 1024
        ),
    )(hidden, head_matrix, targets.reshape(1, rows))
    return result.reshape(rows)


def solution(mesh):
    return jax.shard_map(
        local,
        mesh=mesh,
        in_specs=(P(("vocab", "seq"), None), P("seq", "vocab"), P(("vocab", "seq"))),
        out_specs=P(("vocab", "seq")),
        check_vma=False,
    )
```

```python
import functools

import jax
import jax.numpy as jnp
from jax import lax
from jax.experimental import pallas as pl
from jax.experimental.pallas import tpu as pltpu
from jax.sharding import PartitionSpec as P

MESH = pl.DeviceIdType.MESH
TILE = 256


def ring_index(position, n):
    half = n // 2
    p = lax.rem(position + 2 * n, n)
    low = p // half
    high = jnp.where(low == 0, p, n - 1 - p)
    return high * 2 + low


def kernel(
    n, hidden, head, targets, out,
    x, w, wanted, part, other, stats, gathered,
    local_sem, swap_tx, swap_rx, ring_tx, ring_rx, part_tx, part_rx, far_tx, far_rx, stat_tx, stat_rx,
):
    half = n // 2
    width = head.shape[0]
    columns = head.shape[1]
    rows = hidden.shape[0]
    tile = min(TILE, columns)
    v = lax.axis_index("vocab")
    s = lax.axis_index("seq")
    y, c = s // 2, lax.rem(s, 2)
    low, high = lax.rem(v, 2), v // 2
    position = jnp.where(low == 0, high, n - 1 - high)
    ring = ((ring_index(position + 1, n), s), (ring_index(position - 1, n), s))
    y_mate = (v, (1 - y) * 2 + c)
    c_mate = (v, y * 2 + 1 - c)

    barrier = pltpu.get_barrier_semaphore()
    for device in (*ring, y_mate, c_mate):
        pl.semaphore_signal(barrier, inc=1, device_id=device, device_id_type=MESH)

    def remote(src, dst, tx, rx, device):
        return pltpu.make_async_remote_copy(
            src_ref=src, dst_ref=dst, send_sem=tx, recv_sem=rx, device_id=device, device_id_type=MESH
        )

    def block_at(direction, d):
        return ring_index(position - d if direction == 0 else position + d, n)

    def chunk_ref(block, ch):
        if ch == 4:
            return wanted.at[block]
        unit = y if ch < 2 else 1 - y
        return x.at[block, ch % 2, unit]

    def hop(direction, d, ch, src=None):
        dst = chunk_ref(block_at(direction, d), ch)
        return remote(
            dst if src is None else src, dst,
            ring_tx.at[direction, d, ch], ring_rx.at[direction, d + 1, ch], ring[direction],
        )

    def arrived(direction, d, ch):
        dst = chunk_ref(block_at(direction, d), ch)
        remote(dst, dst, ring_tx.at[direction, d - 1, ch], ring_rx.at[direction, d, ch], ring[direction]).wait_recv()

    def hidden_piece(half_y, h):
        start = pl.multiple_of((half_y * 2 + h) * width, width)
        return hidden.at[:, pl.ds(start, width)]

    own = [
        pltpu.make_async_copy(head, w.at[c], local_sem.at[0]),
        pltpu.make_async_copy(targets, wanted.at[v], local_sem.at[1]),
    ]
    for h in range(2):
        own.append(pltpu.make_async_copy(hidden_piece(y, h), x.at[v, h, y], local_sem.at[2 + h]))
    for copy in own:
        copy.start()
    pl.semaphore_wait(barrier, 4)
    for h in range(2):
        for direction in range(2):
            hop(direction, 0, h, hidden_piece(y, h)).start()
    swaps = [
        remote(hidden_piece(1 - y, h), x.at[v, h, y], swap_tx.at[h], swap_rx.at[h], y_mate) for h in range(2)
    ]
    for swap in swaps:
        swap.start()
    for direction in range(2):
        hop(direction, 0, 4, targets).start()
    head_swap = remote(head, w.at[c], swap_tx.at[2], swap_rx.at[2], c_mate)
    head_swap.start()

    def multiply(block):
        @pl.loop(0, columns // tile)
        def _(j):
            at = pl.ds(pl.multiple_of(j * tile, tile), tile)
            total = None
            for h in range(2):
                term = jnp.dot(
                    x[block, h].reshape(2 * rows, width), w[h, :, at], preferred_element_type=jnp.float32
                )
                total = term if total is None else total + term
            part[block, :, :, at] = total.reshape(2, rows, tile)

    def multiply_tile(blocks, unit, j):
        at = pl.ds(j * tile if isinstance(j, int) else pl.multiple_of(j * tile, tile), tile)
        total = None
        for h in range(2):
            lines = [x[block, h, unit] for block in blocks]
            term = jnp.dot(
                lines[0] if len(lines) == 1 else jnp.concatenate(lines, axis=0),
                w[h, :, at],
                preferred_element_type=jnp.float32,
            )
            total = term if total is None else total + term
        for i, block in enumerate(blocks):
            part[block, unit, :, at] = total[i * rows : (i + 1) * rows]

    def multiply_units(blocks, unit):
        @pl.loop(0, columns // tile)
        def _(j):
            multiply_tile(blocks, unit, j)

    def part_copy(block):
        return remote(part.at[block, 1 - y], other.at[block], part_tx.at[block], part_rx.at[block], y_mate)

    def far_copy(block, j):
        at = pl.ds(j * tile, tile)
        return remote(
            part.at[block, 1 - y, :, at], other.at[block, :, at], far_tx.at[j], far_rx.at[j], y_mate
        )

    def stat_copy(block):
        return remote(stats.at[block], gathered.at[v], stat_tx.at[block], stat_rx.at[v], (block, s))

    def row_stats(block):
        logits = part[block, y] + other[block]
        maximum = jnp.max(logits, axis=1, keepdims=True)
        expsum = jnp.sum(jnp.exp(logits - maximum), axis=1, keepdims=True)
        diagonal = lax.broadcasted_iota(jnp.int32, (rows, rows), 0) == lax.broadcasted_iota(
            jnp.int32, (rows, rows), 1
        )
        target = jnp.sum(jnp.where(diagonal, wanted[block], 0), axis=1, keepdims=True)
        column = lax.broadcasted_iota(jnp.int32, logits.shape, 1) + v * columns
        picked = jnp.sum(jnp.where(column == target, logits, 0.0), axis=1, keepdims=True)
        maximum, expsum, picked = (
            jnp.sum(jnp.where(diagonal, values, 0.0), axis=0, keepdims=True)
            for values in (maximum, expsum, picked)
        )
        line = lax.broadcasted_iota(jnp.int32, (8, rows), 0)
        return jnp.where(line == 0, maximum, jnp.where(line == 1, expsum, picked))

    def give_stats(block):
        part_copy(block).wait_recv()
        stats[block] = row_stats(block)
        stat_copy(block).start()

    for h in range(2):
        swaps[h].wait_recv()
        for direction in range(2):
            hop(direction, 0, 2 + h).start()
    for copy in own:
        copy.wait()
    head_swap.wait_recv()
    multiply(v)
    part_copy(v).start()

    def pass_on(d, chunks):
        for ch in chunks:
            for direction in range(2):
                arrived(direction, d, ch)
                hop(direction, d, ch).start()

    def pair(d):
        return [block_at(direction, d) for direction in range(2)]

    def compute_theirs(d):
        multiply_units(pair(d), 1 - y)
        for block in pair(d):
            part_copy(block).start()

    def compute_ours(d):
        multiply_units(pair(d), y)

    pass_on(1, (4, 0, 2, 3, 1))
    compute_theirs(1)
    compute_ours(1)
    part_copy(v).wait_recv()
    gathered[v] = row_stats(v)

    last = half - 1
    ahead = last - 1

    @pl.loop(2, ahead)
    def _(d):
        pass_on(d, (4, 2, 3))
        compute_theirs(d)
        pass_on(d, (0, 1))
        compute_ours(d)
        for block in pair(d - 1):
            give_stats(block)

    far = block_at(0, half)
    final = ((4, 2, 0), (3, 1))
    pass_on(ahead, (4, 2, 3))
    compute_theirs(ahead)
    for direction in range(2):
        for ch in (0, 1):
            arrived(direction, ahead, ch)
    hop(1, ahead, 1).start()
    for direction in range(2):
        arrived(direction, last, 4)
    hop(0, last, 4).start()
    arrived(0, last, 2)
    hop(0, last, 2).start()
    hop(0, ahead, 0).start()
    hop(0, ahead, 1).start()
    compute_ours(ahead)
    arrived(1, last, 2)
    arrived(1, last, 3)
    hop(1, last, 3).start()
    hop(1, ahead, 0).start()
    arrived(0, last, 3)
    compute_theirs(last)
    for block in pair(ahead - 1):
        give_stats(block)
    arrived(1, last, 1)
    hop(1, last, 1).start()
    for block in pair(ahead):
        give_stats(block)
    arrived(0, last, 0)
    hop(0, last, 0).start()
    arrived(0, half, 4)
    arrived(0, half, 2)
    arrived(1, half, 3)
    for j in range(columns // tile):
        multiply_tile([far], 1 - y, j)
        if j > 0:
            far_copy(far, j - 1).start()
    far_copy(far, columns // tile - 1).start()
    arrived(0, last, 1)
    arrived(1, last, 0)
    compute_ours(last)
    for block in pair(last):
        give_stats(block)
    arrived(0, half, 0)
    arrived(1, half, 1)
    multiply_units([far], y)
    for j in range(columns // tile):
        far_copy(far, j).wait_recv()
    stats[far] = row_stats(far)
    stat_copy(far).start()

    for swap in (*swaps, head_swap):
        swap.wait_send()

    @pl.loop(0, last)
    def _(d):
        for direction in range(2):
            for ch in range(5):
                hop(direction, d, ch).wait_send()

    for direction in range(2):
        for ch in final[direction]:
            hop(direction, last, ch).wait_send()

    for j in range(columns // tile):
        far_copy(far, j).wait_send()
    part_copy(v).wait_send()

    @pl.loop(1, half)
    def _(d):
        for block in pair(d):
            part_copy(block).wait_send()

    @pl.loop(1, n)
    def _(d):
        stat_copy(block_at(0, d)).wait_send()
        peer = block_at(0, d)
        remote(
            stats.at[peer], gathered.at[peer], stat_tx.at[peer], stat_rx.at[peer], (peer, s)
        ).wait_recv()

    maxima, expsums, picked = (gathered[:, i, :] for i in range(3))
    maximum = jnp.max(maxima, axis=0, keepdims=True)
    expsum = jnp.sum(expsums * jnp.exp(maxima - maximum), axis=0, keepdims=True)
    out[...] = jnp.sum(picked, axis=0, keepdims=True) - (maximum + jnp.log(expsum))


def local(hidden, head_matrix, targets):
    n = lax.axis_size("vocab")
    half = n // 2
    rows = hidden.shape[0]
    width, columns = head_matrix.shape
    dma = pltpu.SemaphoreType.DMA
    result = pl.pallas_call(
        functools.partial(kernel, n),
        out_shape=jax.ShapeDtypeStruct((1, rows), jnp.float32),
        in_specs=[pl.BlockSpec(memory_space=pl.ANY)] * 3,
        out_specs=pl.BlockSpec(memory_space=pltpu.VMEM),
        scratch_shapes=[
            pltpu.VMEM((n, 2, 2, rows, width), jnp.bfloat16),
            pltpu.VMEM((2, width, columns), jnp.bfloat16),
            pltpu.VMEM((n, 1, rows), jnp.int32),
            pltpu.VMEM((n, 2, rows, columns), jnp.float32),
            pltpu.VMEM((n, rows, columns), jnp.float32),
            pltpu.VMEM((n, 8, rows), jnp.float32),
            pltpu.VMEM((n, 8, rows), jnp.float32),
            dma((4,)),
            dma((3,)),
            dma((3,)),
            dma((2, half, 5)),
            dma((2, half + 1, 5)),
            dma((n,)),
            dma((n,)),
            dma((columns // min(TILE, columns),)),
            dma((columns // min(TILE, columns),)),
            dma((n,)),
            dma((n,)),
        ],
        compiler_params=pltpu.CompilerParams(
            collective_id=0, has_side_effects=True, vmem_limit_bytes=62 * 1024 * 1024
        ),
    )(hidden, head_matrix, targets.reshape(1, rows))
    return result.reshape(rows)


def solution(mesh):
    return jax.shard_map(
        local,
        mesh=mesh,
        in_specs=(P(("vocab", "seq"), None), P("seq", "vocab"), P(("vocab", "seq"))),
        out_specs=P(("vocab", "seq")),
        check_vma=False,
    )
```

```python
import functools

import jax
import jax.numpy as jnp
from jax import lax
from jax.experimental import pallas as pl
from jax.experimental.pallas import tpu as pltpu
from jax.sharding import PartitionSpec as P

MESH = pl.DeviceIdType.MESH
TILE = 256


def ring_index(position, n):
    half = n // 2
    p = lax.rem(position + 2 * n, n)
    low = p // half
    high = jnp.where(low == 0, p, n - 1 - p)
    return high * 2 + low


def kernel(
    n, hidden, head, targets, out,
    x, w, wanted, part, other, stats, gathered,
    local_sem, swap_tx, swap_rx, ring_tx, ring_rx, part_tx, part_rx, far_tx, far_rx, stat_tx, stat_rx,
):
    half = n // 2
    width = head.shape[0]
    columns = head.shape[1]
    rows = hidden.shape[0]
    tile = min(TILE, columns)
    v = lax.axis_index("vocab")
    s = lax.axis_index("seq")
    y, c = s // 2, lax.rem(s, 2)
    low, high = lax.rem(v, 2), v // 2
    position = jnp.where(low == 0, high, n - 1 - high)
    ring = ((ring_index(position + 1, n), s), (ring_index(position - 1, n), s))
    y_mate = (v, (1 - y) * 2 + c)
    c_mate = (v, y * 2 + 1 - c)

    barrier = pltpu.get_barrier_semaphore()
    for device in (*ring, y_mate, c_mate):
        pl.semaphore_signal(barrier, inc=1, device_id=device, device_id_type=MESH)

    def remote(src, dst, tx, rx, device):
        return pltpu.make_async_remote_copy(
            src_ref=src, dst_ref=dst, send_sem=tx, recv_sem=rx, device_id=device, device_id_type=MESH
        )

    def block_at(direction, d):
        return ring_index(position - d if direction == 0 else position + d, n)

    def chunk_ref(block, ch):
        if ch == 4:
            return wanted.at[block]
        unit = y if ch < 2 else 1 - y
        return x.at[block, ch % 2, unit]

    def hop(direction, d, ch, src=None):
        dst = chunk_ref(block_at(direction, d), ch)
        return remote(
            dst if src is None else src, dst,
            ring_tx.at[direction, d, ch], ring_rx.at[direction, d + 1, ch], ring[direction],
        )

    def arrived(direction, d, ch):
        dst = chunk_ref(block_at(direction, d), ch)
        remote(dst, dst, ring_tx.at[direction, d - 1, ch], ring_rx.at[direction, d, ch], ring[direction]).wait_recv()

    def hidden_piece(half_y, h):
        start = pl.multiple_of((half_y * 2 + h) * width, width)
        return hidden.at[:, pl.ds(start, width)]

    pieces = [pltpu.make_async_copy(hidden_piece(y, h), x.at[v, h, y], local_sem.at[2 + h]) for h in range(2)]
    own = [
        pltpu.make_async_copy(head, w.at[c], local_sem.at[0]),
        pltpu.make_async_copy(targets, wanted.at[v], local_sem.at[1]),
    ]
    for copy in (*pieces, *own):
        copy.start()
    pl.semaphore_wait(barrier, 4)
    for h in range(2):
        pieces[h].wait()
        for direction in range(2):
            hop(direction, 0, h).start()
    swaps = [
        remote(hidden_piece(1 - y, h), x.at[v, h, y], swap_tx.at[h], swap_rx.at[h], y_mate) for h in range(2)
    ]
    for swap in swaps:
        swap.start()
    for direction in range(2):
        hop(direction, 0, 4, targets).start()
    head_swap = remote(head, w.at[c], swap_tx.at[2], swap_rx.at[2], c_mate)
    head_swap.start()

    def multiply(block):
        @pl.loop(0, columns // tile)
        def _(j):
            at = pl.ds(pl.multiple_of(j * tile, tile), tile)
            total = None
            for h in range(2):
                term = jnp.dot(
                    x[block, h].reshape(2 * rows, width), w[h, :, at], preferred_element_type=jnp.float32
                )
                total = term if total is None else total + term
            part[block, :, :, at] = total.reshape(2, rows, tile)

    def multiply_tile(blocks, unit, j):
        at = pl.ds(j * tile if isinstance(j, int) else pl.multiple_of(j * tile, tile), tile)
        total = None
        for h in range(2):
            lines = [x[block, h, unit] for block in blocks]
            term = jnp.dot(
                lines[0] if len(lines) == 1 else jnp.concatenate(lines, axis=0),
                w[h, :, at],
                preferred_element_type=jnp.float32,
            )
            total = term if total is None else total + term
        for i, block in enumerate(blocks):
            part[block, unit, :, at] = total[i * rows : (i + 1) * rows]

    def multiply_units(blocks, unit):
        @pl.loop(0, columns // tile)
        def _(j):
            multiply_tile(blocks, unit, j)

    def part_copy(block):
        return remote(part.at[block, 1 - y], other.at[block], part_tx.at[block], part_rx.at[block], y_mate)

    def far_copy(block, j):
        at = pl.ds(j * tile, tile)
        return remote(
            part.at[block, 1 - y, :, at], other.at[block, :, at], far_tx.at[j], far_rx.at[j], y_mate
        )

    def stat_copy(block):
        return remote(stats.at[block], gathered.at[v], stat_tx.at[block], stat_rx.at[v], (block, s))

    def row_stats(block):
        logits = part[block, y] + other[block]
        maximum = jnp.max(logits, axis=1, keepdims=True)
        expsum = jnp.sum(jnp.exp(logits - maximum), axis=1, keepdims=True)
        diagonal = lax.broadcasted_iota(jnp.int32, (rows, rows), 0) == lax.broadcasted_iota(
            jnp.int32, (rows, rows), 1
        )
        target = jnp.sum(jnp.where(diagonal, wanted[block], 0), axis=1, keepdims=True)
        column = lax.broadcasted_iota(jnp.int32, logits.shape, 1) + v * columns
        picked = jnp.sum(jnp.where(column == target, logits, 0.0), axis=1, keepdims=True)
        maximum, expsum, picked = (
            jnp.sum(jnp.where(diagonal, values, 0.0), axis=0, keepdims=True)
            for values in (maximum, expsum, picked)
        )
        line = lax.broadcasted_iota(jnp.int32, (8, rows), 0)
        return jnp.where(line == 0, maximum, jnp.where(line == 1, expsum, picked))

    def give_stats(block):
        part_copy(block).wait_recv()
        stats[block] = row_stats(block)
        stat_copy(block).start()

    for h in range(2):
        swaps[h].wait_recv()
        for direction in range(2):
            hop(direction, 0, 2 + h).start()
    for copy in own:
        copy.wait()
    head_swap.wait_recv()
    multiply(v)
    part_copy(v).start()

    def pass_on(d, chunks):
        for ch in chunks:
            for direction in range(2):
                arrived(direction, d, ch)
                hop(direction, d, ch).start()

    def pair(d):
        return [block_at(direction, d) for direction in range(2)]

    def compute_theirs(d):
        multiply_units(pair(d), 1 - y)
        for block in pair(d):
            part_copy(block).start()

    def compute_ours(d):
        multiply_units(pair(d), y)

    pass_on(1, (4, 0, 2, 3, 1))
    compute_theirs(1)
    compute_ours(1)
    part_copy(v).wait_recv()
    gathered[v] = row_stats(v)

    last = half - 1
    ahead = last - 1

    @pl.loop(2, ahead)
    def _(d):
        pass_on(d, (4, 2, 3))
        compute_theirs(d)
        pass_on(d, (0, 1))
        compute_ours(d)
        for block in pair(d - 1):
            give_stats(block)

    far = block_at(0, half)
    final = ((4, 2, 0), (3, 1))
    pass_on(ahead, (4, 2, 3))
    compute_theirs(ahead)
    for direction in range(2):
        for ch in (0, 1):
            arrived(direction, ahead, ch)
    hop(1, ahead, 1).start()
    for direction in range(2):
        arrived(direction, last, 4)
    hop(0, last, 4).start()
    arrived(0, last, 2)
    hop(0, last, 2).start()
    hop(0, ahead, 0).start()
    hop(0, ahead, 1).start()
    compute_ours(ahead)
    arrived(1, last, 2)
    arrived(1, last, 3)
    hop(1, last, 3).start()
    hop(1, ahead, 0).start()
    arrived(0, last, 3)
    compute_theirs(last)
    for block in pair(ahead - 1):
        give_stats(block)
    arrived(1, last, 1)
    hop(1, last, 1).start()
    for block in pair(ahead):
        give_stats(block)
    arrived(0, last, 0)
    hop(0, last, 0).start()
    arrived(0, half, 4)
    arrived(0, half, 2)
    arrived(1, half, 3)
    for j in range(columns // tile):
        multiply_tile([far], 1 - y, j)
        if j > 0:
            far_copy(far, j - 1).start()
    far_copy(far, columns // tile - 1).start()
    arrived(0, last, 1)
    arrived(1, last, 0)
    compute_ours(last)
    for block in pair(last):
        give_stats(block)
    arrived(0, half, 0)
    arrived(1, half, 1)
    multiply_units([far], y)
    for j in range(columns // tile):
        far_copy(far, j).wait_recv()
    stats[far] = row_stats(far)
    stat_copy(far).start()

    for swap in (*swaps, head_swap):
        swap.wait_send()

    @pl.loop(0, last)
    def _(d):
        for direction in range(2):
            for ch in range(5):
                hop(direction, d, ch).wait_send()

    for direction in range(2):
        for ch in final[direction]:
            hop(direction, last, ch).wait_send()

    for j in range(columns // tile):
        far_copy(far, j).wait_send()
    part_copy(v).wait_send()

    @pl.loop(1, half)
    def _(d):
        for block in pair(d):
            part_copy(block).wait_send()

    @pl.loop(1, n)
    def _(d):
        stat_copy(block_at(0, d)).wait_send()
        peer = block_at(0, d)
        remote(
            stats.at[peer], gathered.at[peer], stat_tx.at[peer], stat_rx.at[peer], (peer, s)
        ).wait_recv()

    maxima, expsums, picked = (gathered[:, i, :] for i in range(3))
    maximum = jnp.max(maxima, axis=0, keepdims=True)
    expsum = jnp.sum(expsums * jnp.exp(maxima - maximum), axis=0, keepdims=True)
    out[...] = jnp.sum(picked, axis=0, keepdims=True) - (maximum + jnp.log(expsum))


def local(hidden, head_matrix, targets):
    n = lax.axis_size("vocab")
    half = n // 2
    rows = hidden.shape[0]
    width, columns = head_matrix.shape
    dma = pltpu.SemaphoreType.DMA
    result = pl.pallas_call(
        functools.partial(kernel, n),
        out_shape=jax.ShapeDtypeStruct((1, rows), jnp.float32),
        in_specs=[pl.BlockSpec(memory_space=pl.ANY)] * 3,
        out_specs=pl.BlockSpec(memory_space=pltpu.VMEM),
        scratch_shapes=[
            pltpu.VMEM((n, 2, 2, rows, width), jnp.bfloat16),
            pltpu.VMEM((2, width, columns), jnp.bfloat16),
            pltpu.VMEM((n, 1, rows), jnp.int32),
            pltpu.VMEM((n, 2, rows, columns), jnp.float32),
            pltpu.VMEM((n, rows, columns), jnp.float32),
            pltpu.VMEM((n, 8, rows), jnp.float32),
            pltpu.VMEM((n, 8, rows), jnp.float32),
            dma((4,)),
            dma((3,)),
            dma((3,)),
            dma((2, half, 5)),
            dma((2, half + 1, 5)),
            dma((n,)),
            dma((n,)),
            dma((columns // min(TILE, columns),)),
            dma((columns // min(TILE, columns),)),
            dma((n,)),
            dma((n,)),
        ],
        compiler_params=pltpu.CompilerParams(
            collective_id=0, has_side_effects=True, vmem_limit_bytes=62 * 1024 * 1024
        ),
    )(hidden, head_matrix, targets.reshape(1, rows))
    return result.reshape(rows)


def solution(mesh):
    return jax.shard_map(
        local,
        mesh=mesh,
        in_specs=(P(("vocab", "seq"), None), P("seq", "vocab"), P(("vocab", "seq"))),
        out_specs=P(("vocab", "seq")),
        check_vma=False,
    )
```
